32 devices in a mesh: dp: 8 (over y, x, core), expert: 4 (over z).
Axes of the slice: x: 2, y: 2, z: 4, core: 2. Of those that a mesh axis runs over, the one named last changes fastest.
Arguments:
- tokens: bfloat16 [4096, 2048], P(('dp', 'expert')), may hold values from -6 to 6
- routes: int32 [4096, 2], P(('dp', 'expert')), may hold values from 0 to 3, as said below
- grad_hidden: bfloat16 [4096, 2, 768], P(('dp', 'expert')), may hold values from -1.1953125 to 1.1953125
- w_gate: bfloat16 [4, 2048, 768], P('expert'), may hold values from -0.125 to 0.125
- w_up: bfloat16 [4, 2048, 768], P('expert'), may hold values from -0.125 to 0.125
Outputs:
- grad_tokens: bfloat16 [4096, 2048], P(('dp', 'expert'))
- grad_gate: float32 [4, 2048, 768], P('expert', 'dp')
- grad_up: float32 [4, 2048, 768], P('expert', 'dp')
The draws below stay inside these ranges and needn't reach their ends.
Inputs may be any that keep to these rules, and one draw needn't show every extreme that they name: `routes`: each row names 2 different experts. In each data group 2 experts are hot, the same for all rows of the group: in the rows of one device each hot expert of its group is named more often than every other expert and at most 73 times, every other expert at most 64 times. In the rows of every device some expert is named exactly 64 times; in the rows of some device a hot expert is named exactly 73 times. Every expert is hot in some data group. The indices of a group's two hot experts never differ by 2.
All inputs are finite; a program needn't handle non-finite values.
Results may differ from the reference program's by a relative error of at most 0.012.
Values may be sent and summed in bfloat16 or wider, within the bound.
A program may use at most 128 MiB of HBM per device.

```python
import jax
import jax.numpy as jnp
from jax import lax

D = 2048
FF = 768
TOP = 2
TOK_DEV = 128
EXPERTS = 4
DATA_GROUPS = 8
ROW_TOKENS = 512
TOKENS = 4096
COLD = 64
HMAX = 73
N_EXPERT = 4


def draw_routes(key, part):
    nblock = TOKENS // TOK_DEV
    pair_count = TOK_DEV * TOP
    cold_top = pair_count // EXPERTS
    cold_floor = cold_top - 2 - cold_top // 8
    subkeys = jax.random.split(key, 9)
    expert_ids = jnp.arange(EXPERTS, dtype=jnp.int32)
    block_ids = jnp.arange(nblock, dtype=jnp.int32)
    group_ids = block_ids // EXPERTS
    rotation = jax.random.randint(subkeys[0], (), 0, EXPERTS)
    first_hot = (rotation + group_ids) % EXPERTS
    group_offset = jax.random.randint(subkeys[1], (DATA_GROUPS,), 1, EXPERTS // 2)
    offset = group_offset[group_ids]
    second_hot = (first_hot + offset) % EXPERTS
    hot_one = expert_ids[None, :] == first_hot[:, None]
    hot_two = expert_ids[None, :] == second_hot[:, None]
    hot_flag = hot_one | hot_two
    load_table = jax.random.randint(subkeys[2], (nblock, EXPERTS), cold_floor, cold_top - 1)
    scores = jax.random.randint(subkeys[3], (nblock, EXPERTS), 0, 1 << 20) * EXPERTS + expert_ids[None, :]
    scores = jnp.where(hot_flag, -1, scores)
    forced = jnp.argmax(scores, axis=1).astype(jnp.int32)
    special = jax.random.randint(subkeys[4], (), 0, nblock)
    at_special = block_ids == special
    load_table = jnp.where(at_special[:, None], cold_floor, load_table)
    load_table = jnp.where(expert_ids[None, :] == forced[:, None], cold_top, load_table)
    load_table = jnp.where(hot_flag, 0, load_table)
    hot_total = pair_count - jnp.sum(load_table, axis=1)
    spread = jnp.minimum((hot_total - 2 * cold_top - 2) // 2, cold_top // 4)
    extra_load = jax.random.randint(subkeys[5], (nblock,), 0, spread + 1)
    extra_load = jnp.where(at_special, spread, extra_load)
    larger = (hot_total + 1) // 2 + extra_load
    smaller = hot_total - larger
    flipped = jax.random.randint(subkeys[6], (nblock,), 0, 2) == 1
    load_one = jnp.where(flipped, smaller, larger)
    load_two = jnp.where(flipped, larger, smaller)
    load_table = load_table + jnp.where(hot_one, load_one[:, None], 0) + jnp.where(hot_two, load_two[:, None], 0)

    def tickets(counts):
        return jnp.repeat(expert_ids, counts, total_repeat_length=pair_count)
    ticket_rows = jax.vmap(tickets)(load_table)
    pair_rows = jnp.stack([ticket_rows[:, :TOK_DEV], ticket_rows[:, TOK_DEV:]], axis=2)
    swapped = jax.random.randint(subkeys[7], (nblock, TOK_DEV, 1), 0, 2) == 1
    pair_rows = jnp.where(swapped, pair_rows[:, :, ::-1], pair_rows)

    def shuffle(block_key):
        return jax.random.permutation(block_key, TOK_DEV)
    token_order = jax.vmap(shuffle)(jax.random.split(subkeys[8], nblock))
    pair_rows = jnp.take_along_axis(pair_rows, token_order[:, :, None], axis=1)
    return pair_rows.reshape(TOKENS, TOP).astype(jnp.int32)


def shard_levels(key, shape, cuts, least, high):
    factor_of = 1.0
    for position, parts in cuts:
        draws = jax.random.uniform(jax.random.fold_in(jax.random.fold_in(key, 6), position), (parts,), jnp.float32, least / len(cuts), high / len(cuts))
        factor_of = factor_of * jnp.repeat(jnp.exp(draws), shape[position] // parts).reshape((-1,) + (1,) * (len(shape) - 1 - position))
    return factor_of


def normal_values(rng, extent, scale, limit, cuts=(), kind=jnp.bfloat16):
    result = jax.random.normal(rng, extent, jnp.float32) * scale
    if len(cuts) > 0:
        result = shard_levels(rng, extent, cuts, -0.22, 0.18) * result
    return jnp.clip(result, min=-limit, max=limit).astype(kind)


def setup_inputs(seed: int = 0) -> dict:
    streams_of = jax.random.split(jax.random.key(seed), 6)
    return {
        "tokens": normal_values(streams_of[0], (TOKENS, D), 1.0, 6.0, ((0, 32),)),
        "routes": draw_routes(jax.random.fold_in(streams_of[5], 71), 0),
        "grad_hidden": normal_values(streams_of[2], (TOKENS, TOP, FF), 0.2, 1.1953125, ((0, 32),)),
        "w_gate": normal_values(streams_of[3], (EXPERTS, D, FF), D ** -0.5, 0.125, ((0, 4),)),
        "w_up": normal_values(streams_of[4], (EXPERTS, D, FF), D ** -0.5, 0.125, ((0, 4),)),
    }


def expert_grads(rows_x, rows_dh, gate_w, up_w, spill_rows):
    gate_act = jnp.dot(rows_x, gate_w, preferred_element_type=jnp.float32)
    up_act = jnp.dot(rows_x, up_w, preferred_element_type=jnp.float32)
    gate_sig = jax.nn.sigmoid(gate_act)
    grad_wide = rows_dh.astype(jnp.float32)
    gate_delta = (grad_wide * up_act * gate_sig * (1.0 + gate_act * (1.0 - gate_sig))).astype(jnp.bfloat16)
    up_delta = (grad_wide * gate_act * gate_sig).astype(jnp.bfloat16)
    back_rows = lax.dot_general(gate_delta, gate_w, (((1,), (1,)), ((), ())), preferred_element_type=jnp.float32)
    back_rows = back_rows + lax.dot_general(up_delta, up_w, (((1,), (1,)), ((), ())), preferred_element_type=jnp.float32)
    zero_delta = jnp.zeros_like(gate_delta)
    gate_keep = jnp.where(spill_rows[:, None], zero_delta, gate_delta)
    gate_spill = jnp.where(spill_rows[:, None], gate_delta, zero_delta)
    up_keep = jnp.where(spill_rows[:, None], zero_delta, up_delta)
    up_spill = jnp.where(spill_rows[:, None], up_delta, zero_delta)
    dims = (((0,), (0,)), ((), ()))
    grads = tuple(lax.dot_general(rows_x, delta, dims, preferred_element_type=jnp.float32) for delta in (gate_keep, gate_spill, up_keep, up_spill))
    return back_rows.astype(jnp.bfloat16), grads


def reference(tokens, routes, grad_hidden, w_gate, w_up):
    row_pairs = ROW_TOKENS * TOP
    block_rows = 64
    slot_count = row_pairs + EXPERTS * block_rows
    block_count = slot_count // block_rows
    limit_rows = COLD + (HMAX - COLD + 1) // 2
    token_groups = tokens.reshape(DATA_GROUPS, ROW_TOKENS, D)
    route_groups = routes.reshape(DATA_GROUPS, row_pairs)
    grad_groups = grad_hidden.reshape(DATA_GROUPS, row_pairs, FF)
    expert_ids = jnp.arange(EXPERTS, dtype=jnp.int32)

    def one_group(totals, items):
        group_tokens, group_routes, group_grads = items
        device_routes = group_routes.reshape(N_EXPERT, TOK_DEV * TOP)
        member = (device_routes[:, :, None] == expert_ids[None, None, :]).astype(jnp.int32)
        ranked = jnp.sum(jnp.cumsum(member, axis=1) * member, axis=2) - 1
        spill_flag = (ranked >= limit_rows).reshape(row_pairs)
        padded_spill = jnp.concatenate([spill_flag, jnp.zeros((1,), bool)], axis=0)
        counts = jnp.sum((group_routes[:, None] == expert_ids[None, :]).astype(jnp.int32), axis=0)
        padded = (counts + block_rows - 1) // block_rows * block_rows
        offsets = jnp.cumsum(padded) - padded
        starts = jnp.cumsum(counts) - counts
        ordering = jnp.argsort(group_routes, stable=True).astype(jnp.int32)
        sorted_ids = group_routes[ordering]
        slot_of = offsets[sorted_ids] + jnp.arange(row_pairs, dtype=jnp.int32) - starts[sorted_ids]
        slot_table = jnp.full((slot_count,), row_pairs, jnp.int32).at[slot_of].set(ordering)
        end_of = offsets + padded
        block_start = jnp.arange(block_count, dtype=jnp.int32) * block_rows
        block_owner = jnp.minimum(jnp.sum((block_start[:, None] >= end_of[None, :]).astype(jnp.int32), axis=1), EXPERTS - 1)
        padded_tokens = jnp.concatenate([group_tokens, jnp.zeros((1, D), group_tokens.dtype)], axis=0)
        padded_grads = jnp.concatenate([group_grads, jnp.zeros((1, FF), group_grads.dtype)], axis=0)

        def one_block(accums, block_index):
            picked = lax.dynamic_slice_in_dim(slot_table, block_index * block_rows, block_rows)
            tok_index = jnp.where(picked < row_pairs, picked // TOP, ROW_TOKENS).astype(jnp.int32)
            rows_x = padded_tokens[tok_index]
            rows_dh = padded_grads[picked]
            spill_rows = padded_spill[picked]
            expert_now = block_owner[block_index]
            back_rows, grads = expert_grads(rows_x, rows_dh, w_gate[expert_now], w_up[expert_now], spill_rows)
            new_accums = tuple(acc.at[expert_now].add(part) for acc, part in zip(accums, grads))
            return new_accums, back_rows

        zero_grads = jnp.zeros((EXPERTS, D, FF), jnp.float32)
        accums, pair_backs = lax.scan(one_block, (zero_grads, zero_grads, zero_grads, zero_grads), jnp.arange(block_count, dtype=jnp.int32))
        pair_back = jnp.zeros((row_pairs + 1, D), jnp.bfloat16).at[slot_table].set(pair_backs.reshape(slot_count, D))[:row_pairs]
        rounded = [lax.optimization_barrier(acc.astype(jnp.bfloat16)).astype(jnp.float32) for acc in accums]
        return (totals[0] + rounded[0] + rounded[1], totals[1] + rounded[2] + rounded[3]), pair_back

    zero_grads = jnp.zeros((EXPERTS, D, FF), jnp.float32)
    grads, pair_backs = lax.scan(one_group, (zero_grads, zero_grads), (token_groups, route_groups, grad_groups))
    pair_backs = lax.optimization_barrier(pair_backs)
    grad_tokens = jnp.sum(pair_backs.reshape(TOKENS, TOP, D).astype(jnp.float32), axis=1).astype(jnp.bfloat16)
    return grad_tokens, grads[0], grads[1]
```

```python
import functools

import jax
import jax.numpy as jnp
from jax import lax
from jax.experimental import pallas as pl
from jax.experimental.pallas import tpu as pltpu
from jax.sharding import PartitionSpec as P

MESH = pl.DeviceIdType.MESH
BF = jnp.bfloat16
F32 = jnp.float32


def dot(a, b, da, db):
    return lax.dot_general(a, b, (((da,), (db,)), ((), ())), preferred_element_type=F32)


def rs_plan(bits):
    orders = (tuple(range(bits)), (0,) + tuple(range(bits - 1, 0, -1)))
    index = {}
    for which, order in enumerate(orders):
        done = 1
        for bit in order[1:]:
            flag = 1 << bit
            for mask in range(1 << bits):
                if mask & done or mask & flag:
                    continue
                index[which, bit, mask] = len(index)
            done |= flag
    return orders, index


def kernel(
    groups, ways, cap, tok_ref, rt_ref, gh0_ref, gh1_ref, wg_hbm, wu_hbm,
    out_tok, out_gate, out_up,
    wg, wu, pick, send, rows, delta, back, ret, core_send, core_recv, hop_send, hop_recv, acc,
    w_sem, z_ssem, z_rsem, b_ssem, b_rsem, c_ssem, c_rsem, h_ssem, h_rsem,
):
    features = tok_ref.shape[1]
    toks = tok_ref.shape[0]
    hidden = gh0_ref.shape[1]
    block = features // ways
    bits = ways.bit_length() - 1
    orders, index = rs_plan(bits)
    me = lax.axis_index("expert")
    dp = lax.axis_index("dp")
    my_bits = [lax.rem(dp // (1 << b), 2) for b in range(bits)]

    def peer_dp(mask):
        total = 0
        for b in range(bits):
            bit = 1 - my_bits[b] if mask >> b & 1 else my_bits[b]
            total = total + bit * (1 << b)
        return total

    load_g = pltpu.make_async_copy(wg_hbm, wg, w_sem.at[0])
    load_u = pltpu.make_async_copy(wu_hbm, wu, w_sem.at[1])
    load_g.start()
    load_u.start()

    barrier = pltpu.get_barrier_semaphore()
    for off in range(1, groups):
        pl.semaphore_signal(
            barrier, inc=1, device_id={"expert": lax.rem(me + off, groups)}, device_id_type=MESH
        )
    for b in range(bits):
        pl.semaphore_signal(
            barrier, inc=1, device_id={"dp": peer_dp(1 << b)}, device_id_type=MESH
        )

    r0 = rt_ref[0:1, :]
    r1 = rt_ref[1:2, :]
    wide = max(groups, 8)
    ids = lax.broadcasted_iota(jnp.int32, (wide, toks), 0)
    is0 = (ids == r0).astype(F32)
    is1 = (ids == r1).astype(F32)
    before = (
        lax.broadcasted_iota(jnp.int32, (toks, toks), 0)
        < lax.broadcasted_iota(jnp.int32, (toks, toks), 1)
    ).astype(F32).astype(BF)
    earlier = dot((is0 + is1).astype(BF), before, 1, 0)
    pos0 = r0.astype(F32) * cap + jnp.sum(is0 * earlier, axis=0, keepdims=True)
    pos1 = r1.astype(F32) * cap + jnp.sum(is1 * earlier, axis=0, keepdims=True)
    slot = lax.broadcasted_iota(jnp.int32, (groups * cap, toks), 0).astype(F32)
    m0 = (slot == pos0).astype(F32)
    m1 = (slot == pos1).astype(F32)
    pick[...] = (m0 + m1).astype(BF)
    send[:, features:] = (
        dot(m0.astype(BF), gh0_ref[...], 1, 0) + dot(m1.astype(BF), gh1_ref[...], 1, 0)
    ).astype(BF)
    step = 512
    for c in range(0, features, step):
        send[:, c : c + step] = dot(pick[...], tok_ref[:, c : c + step], 1, 0).astype(BF)

    pl.semaphore_wait(barrier, groups - 1 + bits)

    def span(i):
        return pl.ds(pl.multiple_of(i * cap, cap), cap)

    def exchange(src, dst, ssem, rsem):
        sends, recvs = [], []
        for off in range(1, groups):
            to = lax.rem(me + off, groups)
            frm = lax.rem(me + groups - off, groups)
            sends.append(pltpu.make_async_remote_copy(
                src_ref=src.at[span(to)], dst_ref=dst.at[span(me)],
                send_sem=ssem.at[off], recv_sem=rsem.at[off],
                device_id={"expert": to}, device_id_type=MESH))
            recvs.append(pltpu.make_async_remote_copy(
                src_ref=src.at[span(frm)], dst_ref=dst.at[span(frm)],
                send_sem=ssem.at[off], recv_sem=rsem.at[off],
                device_id={"expert": frm}, device_id_type=MESH))
        for copy in sends:
            copy.start()
        return sends, recvs

    out_sends, out_recvs = exchange(send, rows, z_ssem, z_rsem)
    rows[span(me), :] = send[span(me), :]
    load_g.wait()
    load_u.wait()
    for copy in out_recvs:
        copy.wait_recv()

    tile = 256

    def forward(f, carry):
        cols = pl.ds(pl.multiple_of(f * tile, tile), tile)
        ucols = pl.ds(pl.multiple_of(f * tile + hidden, tile), tile)
        dcols = pl.ds(pl.multiple_of(f * tile + features, tile), tile)
        x = rows[:, 0:features]
        gate = dot(x, wg[:, cols], 1, 0)
        up = dot(x, wu[:, cols], 1, 0)
        sig = jax.nn.sigmoid(gate)
        grad = rows[:, dcols].astype(F32)
        delta[:, cols] = (grad * up * sig * (1.0 + gate * (1.0 - sig))).astype(BF)
        delta[:, ucols] = (grad * gate * sig).astype(BF)
        return carry

    lax.fori_loop(0, hidden // tile, forward, 0)

    def weight_block(mask):
        start = pl.multiple_of(peer_dp(mask) * block, block)
        return dot(rows[:, pl.ds(start, block)], delta[...], 0, 0)

    core_sends = {}
    for mask in range(ways - 1, 0, -2):
        place = mask >> 1
        core_send[place] = weight_block(mask).astype(BF)
        copy = pltpu.make_async_remote_copy(
            src_ref=core_send.at[place], dst_ref=core_recv.at[place],
            send_sem=c_ssem.at[place], recv_sem=c_rsem.at[place],
            device_id={"dp": peer_dp(1)}, device_id_type=MESH)
        copy.start()
        core_sends[place] = copy

    def backward(d, carry):
        cols = pl.ds(pl.multiple_of(d * tile, tile), tile)
        back[:, cols] = (
            dot(delta[:, 0:hidden], wg[cols, :], 1, 1)
            + dot(delta[:, hidden:], wu[cols, :], 1, 1)
        ).astype(BF)
        return carry

    lax.fori_loop(0, features // tile, backward, 0)
    back_sends, back_recvs = exchange(back, ret, b_ssem, b_rsem)
    ret[span(me), :] = back[span(me), :]

    hop_sends = []

    def hop(which, bit, mask, value):
        at = index[which, bit, mask ^ (1 << bit)]
        hop_send[at] = value.astype(BF)
        copy = pltpu.make_async_remote_copy(
            src_ref=hop_send.at[at], dst_ref=hop_recv.at[at],
            send_sem=h_ssem.at[at], recv_sem=h_rsem.at[at],
            device_id={"dp": peer_dp(1 << bit)}, device_id_type=MESH)
        copy.start()
        hop_sends.append(copy)

    def arrived(which, bit, mask):
        at = index[which, bit, mask]
        pltpu.make_async_remote_copy(
            src_ref=hop_send.at[at], dst_ref=hop_recv.at[at],
            send_sem=h_ssem.at[at], recv_sem=h_rsem.at[at],
            device_id={"dp": peer_dp(1 << bit)}, device_id_type=MESH).wait_recv()
        return hop_recv[at].astype(F32)

    for mask in range(ways - 2, -1, -2):
        place = mask >> 1
        core_sends[place].wait_recv()
        total = weight_block(mask) + core_recv[place].astype(F32)
        for which in range(2):
            part = total[:, which * hidden : (which + 1) * hidden]
            bit = orders[which][1]
            if mask >> bit & 1:
                hop(which, bit, mask, part)
            else:
                acc[which, place] = part

    for level in range(2, bits):
        for mask in range(ways - 2, -1, -2):
            for which in range(2):
                order = orders[which]
                fixed = sum(1 << b for b in order[:level])
                if mask & fixed:
                    continue
                value = acc[which, mask >> 1] + arrived(which, order[level - 1], mask)
                if mask >> order[level] & 1:
                    hop(which, order[level], mask, value)
                else:
                    acc[which, mask >> 1] = value

    for copy in back_recvs:
        copy.wait_recv()
    for c in range(0, features, step):
        out_tok[:, c : c + step] = dot(pick[...], ret[:, c : c + step], 0, 0).astype(BF)
    out_gate[...] = acc[0, 0] + arrived(0, orders[0][-1], 0)
    out_up[...] = acc[1, 0] + arrived(1, orders[1][-1], 0)

    for copy in out_sends + back_sends + list(core_sends.values()) + hop_sends:
        copy.wait_send()


def per_device(tokens, routes, grad_hidden, w_gate, w_up):
    tok_rows, features = tokens.shape
    per_token = routes.shape[1]
    hidden = w_gate.shape[2]
    groups = lax.axis_size("expert")
    ways = lax.axis_size("dp")
    pair_count = tok_rows * per_token
    cold_most = pair_count // groups
    cold_floor = cold_most - 2 - cold_most // 8
    hot_total = pair_count - (groups - 3) * cold_floor - cold_most
    hot_most = (hot_total + 1) // 2 + min((hot_total - 2 * cold_most - 2) // 2, cold_most // 4)
    cap = (max(hot_most, cold_most) + 15) // 16 * 16
    slots = groups * cap
    block = features // ways
    bits = ways.bit_length() - 1
    hops = len(rs_plan(bits)[1])
    half = ways // 2
    vmem = pl.BlockSpec(memory_space=pltpu.VMEM)
    hbm = pl.BlockSpec(memory_space=pl.ANY)
    dma = pltpu.SemaphoreType.DMA
    tok_grad, gate_grad, up_grad = pl.pallas_call(
        functools.partial(kernel, groups, ways, cap),
        out_shape=(
            jax.ShapeDtypeStruct((tok_rows, features), BF),
            jax.ShapeDtypeStruct((block, hidden), F32),
            jax.ShapeDtypeStruct((block, hidden), F32),
        ),
        in_specs=[vmem, vmem, vmem, vmem, hbm, hbm],
        out_specs=(vmem, vmem, vmem),
        scratch_shapes=[
            pltpu.VMEM((features, hidden), BF),
            pltpu.VMEM((features, hidden), BF),
            pltpu.VMEM((slots, tok_rows), BF),
            pltpu.VMEM((slots, features + hidden), BF),
            pltpu.VMEM((slots, features + hidden), BF),
            pltpu.VMEM((slots, 2 * hidden), BF),
            pltpu.VMEM((slots, features), BF),
            pltpu.VMEM((slots, features), BF),
            pltpu.VMEM((half, block, 2 * hidden), BF),
            pltpu.VMEM((half, block, 2 * hidden), BF),
            pltpu.VMEM((hops, block, hidden), BF),
            pltpu.VMEM((hops, block, hidden), BF),
            pltpu.VMEM((2, half, block, hidden), F32),
            dma((2,)),
            dma((groups,)),
            dma((groups,)),
            dma((groups,)),
            dma((groups,)),
            dma((half,)),
            dma((half,)),
            dma((hops,)),
            dma((hops,)),
        ],
        compiler_params=pltpu.CompilerParams(collective_id=0, has_side_effects=True),
    )(tokens, routes.T, grad_hidden[:, 0], grad_hidden[:, 1], w_gate[0], w_up[0])
    return tok_grad, gate_grad[None], up_grad[None]


def solution(mesh):
    placed = (
        P(("dp", "expert"), None),
        P(("dp", "expert"), None),
        P(("dp", "expert"), None, None),
        P("expert", None, None),
        P("expert", None, None),
    )
    return jax.shard_map(
        per_device,
        mesh=mesh,
        in_specs=placed,
        out_specs=(P(("dp", "expert"), None), P("expert", "dp", None), P("expert", "dp", None)),
        check_vma=False,
    )
```

```python
import functools

import jax
import jax.numpy as jnp
from jax import lax
from jax.experimental import pallas as pl
from jax.experimental.pallas import tpu as pltpu
from jax.sharding import PartitionSpec as P

MESH = pl.DeviceIdType.MESH
BF = jnp.bfloat16
F32 = jnp.float32


def dot(a, b, da, db):
    return lax.dot_general(a, b, (((da,), (db,)), ((), ())), preferred_element_type=F32)


def rs_plan(bits):
    orders = (tuple(range(bits)), (0,) + tuple(range(bits - 1, 0, -1)))
    index = {}
    for which, order in enumerate(orders):
        done = 1
        for bit in order[1:]:
            flag = 1 << bit
            for mask in range(1 << bits):
                if mask & done or mask & flag:
                    continue
                index[which, bit, mask] = len(index)
            done |= flag
    return orders, index


def kernel(
    groups, ways, cap, tile, tok_ref, rt_ref, gh0_ref, gh1_ref, wg_hbm, wu_hbm,
    out_tok, out_gate, out_up,
    wg, wu, pick, send, rows, xt, dsend, drows, delta_g, delta_u, back, ret,
    core_send, core_recv, hop_send, hop_recv, acc,
    w_sem, z_ssem, z_rsem, d_ssem, d_rsem, b_ssem, b_rsem, c_ssem, c_rsem, h_ssem, h_rsem,
):
    features = tok_ref.shape[1]
    toks = tok_ref.shape[0]
    hidden = gh0_ref.shape[1]
    block = features // ways
    slices = hidden // tile
    bits = ways.bit_length() - 1
    orders, index = rs_plan(bits)
    me = lax.axis_index("expert")
    dp = lax.axis_index("dp")
    my_bits = [lax.rem(dp // (1 << b), 2) for b in range(bits)]
    offs = sorted(range(1, groups), key=lambda off: abs(off - groups // 2))

    def peer_dp(mask):
        total = 0
        for b in range(bits):
            bit = 1 - my_bits[b] if mask >> b & 1 else my_bits[b]
            total = total + bit * (1 << b)
        return total

    def span(i):
        return pl.ds(pl.multiple_of(i * cap, cap), cap)

    barrier = pltpu.get_barrier_semaphore()
    for off in range(1, groups):
        pl.semaphore_signal(
            barrier, inc=1, device_id={"expert": lax.rem(me + off, groups)}, device_id_type=MESH
        )
    for b in range(bits):
        pl.semaphore_signal(
            barrier, inc=1, device_id={"dp": peer_dp(1 << b)}, device_id_type=MESH
        )

    r0 = rt_ref[0:1, :]
    r1 = rt_ref[1:2, :]
    wide = max(groups, 8)
    ids = lax.broadcasted_iota(jnp.int32, (wide, toks), 0)
    is0 = (ids == r0).astype(F32)
    is1 = (ids == r1).astype(F32)
    before = (
        lax.broadcasted_iota(jnp.int32, (toks, toks), 0)
        < lax.broadcasted_iota(jnp.int32, (toks, toks), 1)
    ).astype(F32).astype(BF)
    earlier = dot((is0 + is1).astype(BF), before, 1, 0)
    pos0 = r0.astype(F32) * cap + jnp.sum(is0 * earlier, axis=0, keepdims=True)
    pos1 = r1.astype(F32) * cap + jnp.sum(is1 * earlier, axis=0, keepdims=True)
    slot = lax.broadcasted_iota(jnp.int32, (groups * cap, toks), 0).astype(F32)
    m0 = (slot == pos0).astype(F32)
    m1 = (slot == pos1).astype(F32)
    pick[...] = (m0 + m1).astype(BF)

    started = []

    def push(src, dst, ssem, rsem, target):
        copy = pltpu.make_async_remote_copy(
            src_ref=src, dst_ref=dst, send_sem=ssem, recv_sem=rsem,
            device_id=target, device_id_type=MESH)
        copy.start()
        started.append(copy)
        return copy

    def pull(src, dst, ssem, rsem, target):
        pltpu.make_async_remote_copy(
            src_ref=src, dst_ref=dst, send_sem=ssem, recv_sem=rsem,
            device_id=target, device_id_type=MESH).wait_recv()

    step = 512
    ready = False
    for off in offs:
        to = lax.rem(me + off, groups)
        for c in range(0, features, step):
            send[span(to), c : c + step] = dot(
                pick[span(to), :], tok_ref[:, c : c + step], 1, 0
            ).astype(BF)
        if not ready:
            pl.semaphore_wait(barrier, groups - 1 + bits)
            ready = True
        push(send.at[span(to)], rows.at[span(me)], z_ssem.at[off], z_rsem.at[off], {"expert": to})

    for f in range(slices):
        cols = slice(f * tile, (f + 1) * tile)
        dsend[f] = (
            dot(m0.astype(BF), gh0_ref[:, cols], 1, 0)
            + dot(m1.astype(BF), gh1_ref[:, cols], 1, 0)
        ).astype(BF)
        for off in offs:
            to = lax.rem(me + off, groups)
            push(dsend.at[f, span(to)], drows.at[f, span(me)],
                 d_ssem.at[f, off], d_rsem.at[f, off], {"expert": to})
        drows[f, span(me), :] = dsend[f, span(me), :]

    load_g = pltpu.make_async_copy(wg_hbm, wg, w_sem.at[0])
    load_u = pltpu.make_async_copy(wu_hbm, wu, w_sem.at[1])
    load_g.start()
    load_u.start()
    for c in range(0, features, step):
        rows[span(me), c : c + step] = dot(
            pick[span(me), :], tok_ref[:, c : c + step], 1, 0
        ).astype(BF)
    load_g.wait()
    load_u.wait()
    for off in offs:
        frm = lax.rem(me + groups - off, groups)
        pull(send.at[span(frm)], rows.at[span(frm)], z_ssem.at[off], z_rsem.at[off],
             {"expert": frm})

    def flip(d, carry):
        cols = pl.ds(pl.multiple_of(d * 256, 256), 256)
        xt[cols, :] = rows[:, cols].T
        return carry

    def deltas(f):
        cols = slice(f * tile, (f + 1) * tile)
        gate = dot(rows[...], wg[:, cols], 1, 0)
        up = dot(rows[...], wu[:, cols], 1, 0)
        sig = jax.nn.sigmoid(gate)
        if f == 0:
            lax.fori_loop(0, features // 256, flip, 0)
        for off in offs:
            frm = lax.rem(me + groups - off, groups)
            pull(dsend.at[f, span(frm)], drows.at[f, span(frm)],
                 d_ssem.at[f, off], d_rsem.at[f, off], {"expert": frm})
        grad = drows[f].astype(F32)
        delta_g[:, cols] = (grad * up * sig * (1.0 + gate * (1.0 - sig))).astype(BF)
        delta_u[:, cols] = (grad * gate * sig).astype(BF)

    def weight_block(mask, f):
        cols = slice(f * tile, (f + 1) * tile)
        start = pl.multiple_of(peer_dp(mask) * block, block)
        x = xt[pl.ds(start, block), :]
        return dot(x, delta_g[:, cols], 1, 0), dot(x, delta_u[:, cols], 1, 0)

    def core_stage(f):
        for mask in range(ways - 1, 0, -2):
            place = mask >> 1
            gate, up = weight_block(mask, f)
            core_send[f, place, :, 0:tile] = gate.astype(BF)
            core_send[f, place, :, tile:] = up.astype(BF)
            push(core_send.at[f, place], core_recv.at[f, place],
                 c_ssem.at[f, place], c_rsem.at[f, place], {"dp": peer_dp(1)})

    def hop(f, which, bit, mask, value):
        at = index[which, bit, mask ^ (1 << bit)]
        hop_send[f, at] = value.astype(BF)
        push(hop_send.at[f, at], hop_recv.at[f, at], h_ssem.at[f, at], h_rsem.at[f, at],
             {"dp": peer_dp(1 << bit)})

    def arrived(f, which, bit, mask):
        at = index[which, bit, mask]
        pull(hop_send.at[f, at], hop_recv.at[f, at], h_ssem.at[f, at], h_rsem.at[f, at],
             {"dp": peer_dp(1 << bit)})
        return hop_recv[f, at].astype(F32)

    def first_hops(f):
        for mask in range(ways - 2, -1, -2):
            place = mask >> 1
            pull(core_send.at[f, place], core_recv.at[f, place],
                 c_ssem.at[f, place], c_rsem.at[f, place], {"dp": peer_dp(1)})
            parts = weight_block(mask, f)
            for which in range(2):
                other = core_recv[f, place, :, which * tile : (which + 1) * tile]
                part = parts[which] + other.astype(F32)
                bit = orders[which][1]
                if mask >> bit & 1:
                    hop(f, which, bit, mask, part)
                else:
                    acc[f, which, place] = part

    def later_hops(f):
        for level in range(2, bits):
            for mask in range(ways - 2, -1, -2):
                for which in range(2):
                    order = orders[which]
                    if mask & sum(1 << b for b in order[:level]):
                        continue
                    value = acc[f, which, mask >> 1] + arrived(f, which, order[level - 1], mask)
                    if mask >> order[level] & 1:
                        hop(f, which, order[level], mask, value)
                    else:
                        acc[f, which, mask >> 1] = value

    parts = 2
    width = features // parts

    def backward(d, carry):
        cols = pl.ds(pl.multiple_of(d * 256, 256), 256)
        back[:, cols] = (
            dot(delta_g[...], wg[cols, :], 1, 1) + dot(delta_u[...], wu[cols, :], 1, 1)
        ).astype(BF)
        return carry

    def give_back():
        each = width // 256
        for part in range(parts):
            lax.fori_loop(part * each, (part + 1) * each, backward, 0)
            cols = pl.ds(part * width, width)
            for off in offs:
                to = lax.rem(me + off, groups)
                push(back.at[span(to), cols], ret.at[span(me), cols],
                     b_ssem.at[part, off], b_rsem.at[part, off], {"expert": to})

    for f in range(slices):
        deltas(f)
        if f == slices - 1:
            give_back()
        core_stage(f)
        first_hops(f)
        if f > 0:
            later_hops(f - 1)
    later_hops(slices - 1)

    for f in range(slices):
        cols = slice(f * tile, (f + 1) * tile)
        out_gate[:, cols] = acc[f, 0, 0] + arrived(f, 0, orders[0][-1], 0)
        out_up[:, cols] = acc[f, 1, 0] + arrived(f, 1, orders[1][-1], 0)
    ret[span(me), :] = back[span(me), :]
    for part in range(parts):
        cols = pl.ds(part * width, width)
        for off in offs:
            frm = lax.rem(me + groups - off, groups)
            pull(back.at[span(frm), cols], ret.at[span(frm), cols],
                 b_ssem.at[part, off], b_rsem.at[part, off], {"expert": frm})
        for c in range(part * width, (part + 1) * width, step):
            out_tok[:, c : c + step] = dot(pick[...], ret[:, c : c + step], 0, 0).astype(BF)

    for copy in started:
        copy.wait_send()


def settle(*refs):
    srcs, dsts, bufs = refs[0:3], refs[3:6], refs[6:9]
    in_sem, out_sem = refs[9:]
    ins = [pltpu.make_async_copy(s, b, in_sem.at[i]) for i, (s, b) in enumerate(zip(srcs, bufs))]
    outs = [pltpu.make_async_copy(b, d, out_sem.at[i]) for i, (b, d) in enumerate(zip(bufs, dsts))]
    for copy in ins:
        copy.start()
    for first, second in zip(ins, outs):
        first.wait()
        second.start()
    for copy in outs:
        copy.wait()


def per_device(tokens, routes, grad_hidden, w_gate, w_up):
    tok_rows, features = tokens.shape
    per_token = routes.shape[1]
    hidden = w_gate.shape[2]
    groups = lax.axis_size("expert")
    ways = lax.axis_size("dp")
    pair_count = tok_rows * per_token
    cold_most = pair_count // groups
    cold_floor = cold_most - 2 - cold_most // 8
    hot_total = pair_count - (groups - 3) * cold_floor - cold_most
    hot_most = (hot_total + 1) // 2 + min((hot_total - 2 * cold_most - 2) // 2, cold_most // 4)
    cap = (max(hot_most, cold_most) + 15) // 16 * 16
    slots = groups * cap
    block = features // ways
    bits = ways.bit_length() - 1
    hops = len(rs_plan(bits)[1])
    tile = 256
    slices = hidden // tile
    half = ways // 2
    vmem = pl.BlockSpec(memory_space=pltpu.VMEM)
    hbm = pl.BlockSpec(memory_space=pl.ANY)
    dma = pltpu.SemaphoreType.DMA
    tok_grad, gate_grad, up_grad = pl.pallas_call(
        functools.partial(kernel, groups, ways, cap, tile),
        out_shape=(
            jax.ShapeDtypeStruct((tok_rows, features), BF),
            jax.ShapeDtypeStruct((block, hidden), F32),
            jax.ShapeDtypeStruct((block, hidden), F32),
        ),
        in_specs=[vmem, vmem, vmem, vmem, hbm, hbm],
        out_specs=(vmem, vmem, vmem),
        scratch_shapes=[
            pltpu.VMEM((features, hidden), BF),
            pltpu.VMEM((features, hidden), BF),
            pltpu.VMEM((slots, tok_rows), BF),
            pltpu.VMEM((slots, features), BF),
            pltpu.VMEM((slots, features), BF),
            pltpu.VMEM((features, slots), BF),
            pltpu.VMEM((slices, slots, tile), BF),
            pltpu.VMEM((slices, slots, tile), BF),
            pltpu.VMEM((slots, hidden), BF),
            pltpu.VMEM((slots, hidden), BF),
            pltpu.VMEM((slots, features), BF),
            pltpu.VMEM((slots, features), BF),
            pltpu.VMEM((slices, half, block, 2 * tile), BF),
            pltpu.VMEM((slices, half, block, 2 * tile), BF),
            pltpu.VMEM((slices, hops, block, tile), BF),
            pltpu.VMEM((slices, hops, block, tile), BF),
            pltpu.VMEM((slices, 2, half, block, tile), F32),
            dma((2,)),
            dma((groups,)),
            dma((groups,)),
            dma((slices, groups)),
            dma((slices, groups)),
            dma((2, groups)),
            dma((2, groups)),
            dma((slices, half)),
            dma((slices, half)),
            dma((slices, hops)),
            dma((slices, hops)),
        ],
        compiler_params=pltpu.CompilerParams(collective_id=0, has_side_effects=True),
    )(tokens, routes.T, grad_hidden[:, 0], grad_hidden[:, 1], w_gate[0], w_up[0])
    results = (tok_grad, gate_grad, up_grad)
    tok_grad, gate_grad, up_grad = pl.pallas_call(
        settle,
        out_shape=tuple(jax.ShapeDtypeStruct(r.shape, r.dtype) for r in results),
        in_specs=[hbm] * 3,
        out_specs=(hbm,) * 3,
        scratch_shapes=[pltpu.VMEM(r.shape, r.dtype) for r in results] + [dma((3,)), dma((3,))],
    )(*results)
    return tok_grad, gate_grad[None], up_grad[None]


def solution(mesh):
    placed = (
        P(("dp", "expert"), None),
        P(("dp", "expert"), None),
        P(("dp", "expert"), None, None),
        P("expert", None, None),
        P("expert", None, None),
    )
    return jax.shard_map(
        per_device,
        mesh=mesh,
        in_specs=placed,
        out_specs=(P(("dp", "expert"), None), P("expert", "dp", None), P("expert", "dp", None)),
        check_vma=False,
    )
```
